32 devices in a mesh: bank: 8 (over y, x, core), lane: 4 (over z).
Axes of the slice: x: 2, y: 2, z: 4, core: 2. Of those that a mesh axis runs over, the one named last changes fastest.
Arguments:
- amplitudes: float32 [2, 128, 128, 128], P(None, ('bank', 'lane')), may hold values from -6 to 6
- energies: float32 [128, 128, 128], P(('bank', 'lane')), may hold values from -2 to 2
- phase_angles: float32 [2, 128], replicated, may hold values from 0.3 to 1.2
- mix_angles: float32 [2, 4], replicated, may hold values from 0.3 to 1.2
Outputs:
- final_parts: float32 [2, 128, 128, 128], P(None, ('bank', 'lane'))
- marginal: float32 [16, 128, 128], P('lane', 'bank')
The draws below stay inside these ranges and needn't reach their ends.
All inputs are finite; a program needn't handle non-finite values.
Results may differ from the reference program's by a relative error of at most 0.0003.
Values sent between devices are 32-bit elements; how exact they have to be, the bound alone decides.
A program may use at most 64 MiB of HBM per device.

```python
import jax
import jax.numpy as jnp
from jax import lax

BLOCKS_DEV = 4
ROWS = 128
LANES = 128
BLOCKS = 128
LAYERS = 2
N_BANK = 8
N_LANE = 4


def steps_of(stream_key, dims, pieces, low, top_value):
    def one(axis_at, shards_of):
        heights = jax.random.uniform(jax.random.fold_in(jax.random.fold_in(stream_key, 6), axis_at), (shards_of,), jnp.float32, low / len(pieces), top_value / len(pieces))
        return jnp.repeat(jnp.exp(heights), dims[axis_at] // shards_of).reshape((-1,) + (1,) * (len(dims) - axis_at - 1))

    loudness = one(*pieces[0])
    for cut in pieces[1:]:
        loudness = loudness * one(*cut)
    return loudness


def noise(key, dims, spread, bound, shards=(), kind=jnp.bfloat16):
    entries = jax.random.normal(key, dims, jnp.float32) * spread
    if len(shards) > 0:
        entries = steps_of(key, dims, shards, -0.22, 0.18) * entries
    return jnp.clip(entries, min=-bound, max=bound).astype(kind)


def setup_inputs(seed: int = 0) -> dict:
    key_list = jax.random.split(jax.random.key(seed), 5)
    return {
        "amplitudes": noise(key_list[0], (2, BLOCKS, ROWS, LANES), 1.0, 6.0, ((1, 32),), jnp.float32),
        "energies": jnp.clip(jax.random.uniform(key_list[1], (BLOCKS, ROWS, LANES), jnp.float32, -2.0, 2.0) * steps_of(key_list[1], (BLOCKS, ROWS, LANES), ((0, 32),), -0.4, 0.0), -2.0, 2.0),
        "phase_angles": jnp.clip(jax.random.uniform(key_list[2], (LAYERS, LANES), jnp.float32, 0.3, 1.2), 0.3, 1.2),
        "mix_angles": jnp.clip(jax.random.uniform(key_list[3], (LAYERS, 4), jnp.float32, 0.3, 1.2), 0.3, 1.2),
    }


def count_bits(values, count):
    places = jnp.arange(count.bit_length() - 1, dtype=jnp.int32)
    return jnp.sum((values[..., None] >> places) & 1, axis=-1)


def turn_table(count, angle):
    rank = jnp.arange(count, dtype=jnp.int32)
    apart = count_bits(rank[:, None] ^ rank[None, :], count)
    bits = count.bit_length() - 1
    size = jnp.cos(angle) ** (bits - apart).astype(jnp.float32) * jnp.sin(angle) ** apart.astype(jnp.float32)
    real_sign = jnp.where(apart % 4 == 0, 1.0, jnp.where(apart % 4 == 2, -1.0, 0.0)).astype(jnp.float32)
    imag_sign = jnp.where(apart % 4 == 1, -1.0, jnp.where(apart % 4 == 3, 1.0, 0.0)).astype(jnp.float32)
    return size * real_sign, size * imag_sign


def apply_along(values, dim, angle):
    real_part, imag_part = turn_table(values.shape[dim], angle)
    def times(table):
        moved = jnp.tensordot(values, table, axes=([dim], [0]), precision=lax.Precision.HIGHEST)
        return jnp.moveaxis(moved, -1, dim)
    by_real = times(real_part)
    by_imag = times(imag_part)
    return jnp.stack([by_real[0] - by_imag[1], by_real[1] + by_imag[0]])


def diagonal_step(values, levels, angle):
    turn = angle * levels
    return jnp.stack([values[0] * jnp.cos(turn) + values[1] * jnp.sin(turn), values[1] * jnp.cos(turn) - values[0] * jnp.sin(turn)])


def reference(amplitudes, energies, phase_angles, mix_angles):
    values = amplitudes
    for layer in range(LAYERS):
        values = diagonal_step(values, energies, phase_angles[layer])
        values = apply_along(values, 3, mix_angles[layer, 0])
        values = apply_along(values, 2, mix_angles[layer, 1])
        parts = values.reshape(2, N_BANK, N_LANE, BLOCKS_DEV, ROWS, LANES)
        parts = apply_along(parts, 1, mix_angles[layer, 2])
        parts = apply_along(parts, 2, mix_angles[layer, 3])
        parts = apply_along(parts, 3, mix_angles[layer, 2])
        values = parts.reshape(values.shape)
    chance = values[0] * values[0] + values[1] * values[1]
    marginal = jnp.mean(chance.reshape(N_BANK, -1, ROWS, LANES), axis=0)
    return values, marginal
```

```python
import functools

import jax
import jax.numpy as jnp
from jax import lax
from jax.experimental import pallas as pl
from jax.experimental.pallas import tpu as pltpu
from jax.sharding import PartitionSpec as P

MESH = pl.DeviceIdType.MESH
SIN = (1.0, -1 / 6, 1 / 120, -1 / 5040, 1 / 362880, -1 / 39916800, 1 / 6227020800, -1 / 1307674368000)
COS = (1.0, -1 / 2, 1 / 24, -1 / 720, 1 / 40320, -1 / 3628800, 1 / 479001600, -1 / 87178291200, 1 / 20922789888000)


def series(square, terms):
    total = jnp.full_like(square, terms[-1])
    for term in terms[-2::-1]:
        total = total * square + term
    return total


def sin_cos(turn):
    square = turn * turn
    return turn * series(square, SIN), series(square, COS)


def split(x):
    high = x.astype(jnp.bfloat16)
    return high, (x - high.astype(jnp.float32)).astype(jnp.bfloat16)


def dot3(a, b):
    def one(x, y):
        return lax.dot_general(x, y, (((1,), (0,)), ((), ())), preferred_element_type=jnp.float32)

    return one(a[0], b[0]) + (one(a[1], b[0]) + one(a[0], b[1]))


def turn_table(count, cosine, sine):
    row = lax.broadcasted_iota(jnp.int32, (count, count), 0)
    col = lax.broadcasted_iota(jnp.int32, (count, count), 1)
    apart = row ^ col
    size = jnp.ones((count, count), jnp.float32)
    ones = jnp.zeros((count, count), jnp.int32)
    for place in range(count.bit_length() - 1):
        bit = (apart >> place) & 1
        size = size * jnp.where(bit == 1, sine, cosine)
        ones = ones + bit
    phase = ones & 3
    real = jnp.where(phase == 0, size, jnp.where(phase == 2, -size, 0.0))
    imag = jnp.where(phase == 1, -size, jnp.where(phase == 3, size, 0.0))
    return real, imag


def butterfly(re, im, stride, cosine, sine):
    count, rest = re.shape[0], re.shape[1:]
    parts = (count // (2 * stride), 2, stride) + rest
    re, im = re.reshape(parts), im.reshape(parts)
    ur, vr, ui, vi = re[:, 0], re[:, 1], im[:, 0], im[:, 1]
    new_re = jnp.stack([cosine * ur + sine * vi, cosine * vr + sine * ui], axis=1)
    new_im = jnp.stack([cosine * ui - sine * vr, cosine * vi - sine * ur], axis=1)
    return new_re.reshape((count,) + rest), new_im.reshape((count,) + rest)


def kernel(nb, nl, amp, en, ph, mix, out, marg, tmp, s_a, e_b, b_b, o_b, r_a, cs_b, sn_b, ch, m_in, send, recv):
    n = nb * nl
    depth, rows, lanes = amp.shape[1:]
    per = en.shape[1]
    tiled = per % 8 == 0
    units = rows // per
    piece = rows // nb
    bank, lane = lax.axis_index("bank"), lax.axis_index("lane")
    me = bank * nl + lane

    barrier = pltpu.get_barrier_semaphore()

    def greet(k, carry):
        pl.semaphore_signal(
            barrier, 1, device_id=(lax.rem(bank + k // nl, nb), lax.rem(lane + lax.rem(k, nl), nl)), device_id_type=MESH
        )
        return carry

    lax.fori_loop(1, n, greet, 0)
    pl.semaphore_wait(barrier, n - 1)

    def exchange(src, dst, which):
        def one(k, carry):
            to_bank, to_lane = lax.rem(bank + k // nl, nb), lax.rem(lane + lax.rem(k, nl), nl)
            pltpu.make_async_remote_copy(
                src_ref=src.at[to_bank * nl + to_lane],
                dst_ref=dst.at[me],
                send_sem=send.at[which],
                recv_sem=recv.at[which],
                device_id=(to_bank, to_lane),
                device_id_type=MESH,
            ).start()
            return carry

        lax.fori_loop(1, n, one, 0)
        dst[me] = src[me]

    def arrived(dst, count, sems, which):
        most = dst.at[pl.ds(0, count - 1)]
        pltpu.make_async_copy(most, most, sems.at[which]).wait()

    exchange(en, e_b, 0)

    cosines, sines = jnp.cos(mix[...]), jnp.sin(mix[...])

    def angle(layer, group):
        return cosines[layer : layer + 1, group : group + 1], sines[layer : layer + 1, group : group + 1]

    def local_mix(layer, read, write):
        real, imag = turn_table(lanes, *angle(layer, 0))
        by_lane = split(jnp.concatenate([jnp.concatenate([real, imag], 1), jnp.concatenate([-imag, real], 1)], 0))
        real, imag = turn_table(rows, *angle(layer, 1))
        by_row = split(jnp.concatenate([jnp.concatenate([real, -imag], 1), jnp.concatenate([imag, real], 1)], 0))
        pairs = [read(d) for d in range(depth)]
        stride = 1
        cosine, sine = (jnp.broadcast_to(x, (8, lanes))[None] for x in angle(layer, 2))
        re = jnp.stack([p[0] for p in pairs]).reshape(depth, rows // 8, 8, lanes)
        im = jnp.stack([p[1] for p in pairs]).reshape(depth, rows // 8, 8, lanes)
        while stride < depth:
            re, im = butterfly(re, im, stride, cosine, sine)
            stride *= 2
        re, im = re.reshape(depth, rows, lanes), im.reshape(depth, rows, lanes)
        for d in range(depth):
            both = dot3(split(jnp.concatenate([re[d], im[d]], 1)), by_lane)
            both = dot3(by_row, split(jnp.concatenate([both[:, :lanes], both[:, lanes:]], 0)))
            write(d, both[:rows], both[rows:])

    def first(d):
        if tiled:
            e = en[pl.ds(d * units, units)].reshape(rows, lanes)
        else:
            e = tmp[0, d]
        sine, cosine = sin_cos(ph[0:1] * e)
        return amp[0, d] * cosine + amp[1, d] * sine, amp[1, d] * cosine - amp[0, d] * sine

    def to_units(d, re, im):
        if tiled:
            s_a[pl.ds(d * units, units), 0] = re.reshape(units, per, lanes)
            s_a[pl.ds(d * units, units), 1] = im.reshape(units, per, lanes)
        else:
            tmp[0, d] = re
            tmp[1, d] = im

    if not tiled:
        for d in range(depth):

            def spread(u, carry):
                tmp[0, d, pl.ds(u * per, per)] = en[d * units + u]
                return carry

            lax.fori_loop(0, units, spread, 0)
    local_mix(0, first, to_units)
    if not tiled:
        for d in range(depth):

            def gather(u, carry):
                for part in range(2):
                    s_a[d * units + u, part] = tmp[part, d, pl.ds(u * per, per)]
                return carry

            lax.fori_loop(0, units, gather, 0)

    exchange(s_a, b_b, 1)
    arrived(e_b, n, recv, 0)
    sine, cosine = sin_cos(ph[1:2][None] * e_b[...])
    sn_b[...] = sine
    cs_b[...] = cosine
    arrived(b_b, n, recv, 1)

    step = 8 if tiled else per
    for at in range(0, per, step):
        span = pl.ds(at, step)
        re, im = b_b[:, 0, span], b_b[:, 1, span]
        for layer in range(2):
            stride = 1
            while stride < n:
                cosine, sine = (
                    jnp.broadcast_to(x, (step, lanes))[None, None] for x in angle(layer, 3 if stride < nl else 2)
                )
                re, im = butterfly(re, im, stride, cosine, sine)
                stride *= 2
            if layer == 0:
                cosine, sine = cs_b[:, span], sn_b[:, span]
                re, im = re * cosine + im * sine, im * cosine - re * sine
        o_b[:, 0, span] = re
        o_b[:, 1, span] = im

    exchange(o_b, r_a, 2)
    arrived(r_a, n, recv, 2)

    if not tiled:
        for d in range(depth):

            def place(u, carry):
                for part in range(2):
                    tmp[part, d, pl.ds(u * per, per)] = r_a[d * units + u, part]
                return carry

            lax.fori_loop(0, units, place, 0)

    def second(d):
        if tiled:
            return tuple(r_a[pl.ds(d * units, units), part].reshape(rows, lanes) for part in range(2))
        return tmp[0, d], tmp[1, d]

    def finish(d, re, im):
        out[0, d] = re
        out[1, d] = im
        chance = re * re + im * im
        for g in range(nb):
            ch[g, d] = chance[g * piece : (g + 1) * piece]

    local_mix(1, second, finish)

    def pass_on(k, carry):
        to_bank = lax.rem(bank + k, nb)
        pltpu.make_async_remote_copy(
            src_ref=ch.at[to_bank],
            dst_ref=m_in.at[bank],
            send_sem=send.at[3],
            recv_sem=recv.at[3],
            device_id=(to_bank, lane),
            device_id_type=MESH,
        ).start()
        return carry

    lax.fori_loop(1, nb, pass_on, 0)
    m_in[bank] = ch[bank]
    arrived(m_in, nb, recv, 3)
    total = m_in[0]
    for g in range(1, nb):
        total = total + m_in[g]
    marg[...] = total * (1.0 / nb)
    arrived(e_b, n, send, 0)
    arrived(b_b, n, send, 1)
    arrived(r_a, n, send, 2)
    arrived(m_in, nb, send, 3)


def on_device(nb, nl, amplitudes, energies, phase_angles, mix_angles):
    _, depth, rows, lanes = amplitudes.shape
    n = nb * nl
    per = depth * rows // n
    piece = rows // nb
    f32 = jnp.float32
    state = pltpu.VMEM((n, 2, per, lanes), f32)
    level = pltpu.VMEM((n, per, lanes), f32)
    vmem = pl.BlockSpec(memory_space=pltpu.VMEM)
    return pl.pallas_call(
        functools.partial(kernel, nb, nl),
        name="register",
        out_shape=(
            jax.ShapeDtypeStruct(amplitudes.shape, f32),
            jax.ShapeDtypeStruct((depth, piece, lanes), f32),
        ),
        in_specs=[vmem] * 4,
        out_specs=(vmem, vmem),
        scratch_shapes=[
            pltpu.VMEM((2, depth, rows, lanes) if per % 8 else (1, 1, 8, 128), f32),
            state,
            level,
            state,
            state,
            state,
            level,
            level,
            pltpu.VMEM((nb, depth, piece, lanes), f32),
            pltpu.VMEM((nb, depth, piece, lanes), f32),
            pltpu.SemaphoreType.DMA((4,)),
            pltpu.SemaphoreType.DMA((4,)),
        ],
        compiler_params=pltpu.CompilerParams(collective_id=0, has_side_effects=True),
    )(amplitudes, energies.reshape(n, per, lanes), phase_angles, mix_angles)


def solution(mesh):
    placed = (P(None, ("bank", "lane"), None, None), P(("bank", "lane"), None, None), P(), P())
    return jax.shard_map(
        functools.partial(on_device, mesh.shape["bank"], mesh.shape["lane"]),
        mesh=mesh,
        in_specs=placed,
        out_specs=(P(None, ("bank", "lane"), None, None), P("lane", "bank", None)),
        check_vma=False,
    )
```

```python
import functools

import jax
import jax.numpy as jnp
from jax import lax
from jax.experimental import pallas as pl
from jax.experimental.pallas import tpu as pltpu
from jax.sharding import PartitionSpec as P

MESH = pl.DeviceIdType.MESH
SIN = (1.0, -1 / 6, 1 / 120, -1 / 5040, 1 / 362880, -1 / 39916800, 1 / 6227020800, -1 / 1307674368000)
COS = (1.0, -1 / 2, 1 / 24, -1 / 720, 1 / 40320, -1 / 3628800, 1 / 479001600, -1 / 87178291200, 1 / 20922789888000)


def series(square, terms):
    total = jnp.full_like(square, terms[-1])
    for term in terms[-2::-1]:
        total = total * square + term
    return total


def sin_cos(turn):
    square = turn * turn
    return turn * series(square, SIN), series(square, COS)


def split(x):
    high = x.astype(jnp.bfloat16)
    return high, (x - high.astype(jnp.float32)).astype(jnp.bfloat16)


def dot3(a, b):
    def one(x, y):
        return lax.dot_general(x, y, (((1,), (0,)), ((), ())), preferred_element_type=jnp.float32)

    return one(a[0], b[0]) + (one(a[1], b[0]) + one(a[0], b[1]))


def turn_table(count, cosine, sine):
    row = lax.broadcasted_iota(jnp.int32, (count, count), 0)
    col = lax.broadcasted_iota(jnp.int32, (count, count), 1)
    apart = row ^ col
    size = jnp.ones((count, count), jnp.float32)
    ones = jnp.zeros((count, count), jnp.int32)
    for place in range(count.bit_length() - 1):
        bit = (apart >> place) & 1
        size = size * jnp.where(bit == 1, sine, cosine)
        ones = ones + bit
    phase = ones & 3
    real = jnp.where(phase == 0, size, jnp.where(phase == 2, -size, 0.0))
    imag = jnp.where(phase == 1, -size, jnp.where(phase == 3, size, 0.0))
    return real, imag


def butterfly(re, im, stride, cosine, sine):
    count, rest = re.shape[0], re.shape[1:]
    parts = (count // (2 * stride), 2, stride) + rest
    re, im = re.reshape(parts), im.reshape(parts)
    ur, vr, ui, vi = re[:, 0], re[:, 1], im[:, 0], im[:, 1]
    new_re = jnp.stack([cosine * ur + sine * vi, cosine * vr + sine * ui], axis=1)
    new_im = jnp.stack([cosine * ui - sine * vr, cosine * vi - sine * ur], axis=1)
    return new_re.reshape((count,) + rest), new_im.reshape((count,) + rest)


def kernel(
    nb, nl, halves, amp_hbm, en_hbm, ph, mix, out, marg,
    amp, en, tmp, s_a, e_b, b_b, o_b, r_a, cs_b, sn_b, part_done, ch, m_in, load, send, recv,
):
    n = nb * nl
    depth, rows, lanes = amp.shape[1:]
    per = en.shape[1]
    step = per // halves
    tiled = per % 8 == 0
    units = rows // per
    piece = rows // nb
    last = 2 * halves + 1
    bank, lane = lax.axis_index("bank"), lax.axis_index("lane")
    me = bank * nl + lane

    load_en = pltpu.make_async_copy(en_hbm, en, load.at[0])
    load_amp = pltpu.make_async_copy(amp_hbm, amp, load.at[1])
    load_en.start()
    load_amp.start()
    barrier = pltpu.get_barrier_semaphore()

    def partner(k):
        return lax.rem(bank + lax.rem(k, nb), nb), lax.rem(lane + k // nb, nl)

    def greet(k, carry):
        pl.semaphore_signal(barrier, 1, device_id=partner(k), device_id_type=MESH)
        return carry

    lax.fori_loop(1, n, greet, 0)

    def exchange(src, dst, which):
        def one(k, carry):
            to_bank, to_lane = partner(k)
            pltpu.make_async_remote_copy(
                src_ref=src.at[to_bank * nl + to_lane],
                dst_ref=dst.at[me],
                send_sem=send.at[which],
                recv_sem=recv.at[which],
                device_id=(to_bank, to_lane),
                device_id_type=MESH,
            ).start()
            return carry

        lax.fori_loop(1, n, one, 0)
        dst[me] = src[me]

    def arrived(dst, count, sems, which):
        most = dst.at[pl.ds(0, count - 1)]
        pltpu.make_async_copy(most, most, sems.at[which]).wait()

    cosines, sines = jnp.cos(mix[...]), jnp.sin(mix[...])

    def angle(layer, group):
        return cosines[layer : layer + 1, group : group + 1], sines[layer : layer + 1, group : group + 1]

    def tables(layer, count):
        real, imag = turn_table(lanes, *angle(layer, 0))
        by_lane = split(jnp.concatenate([jnp.concatenate([real, imag], 1), jnp.concatenate([-imag, real], 1)], 0))
        real, imag = turn_table(count, *angle(layer, 1))
        by_row = split(jnp.concatenate([jnp.concatenate([real, -imag], 1), jnp.concatenate([imag, real], 1)], 0))
        return by_lane, by_row

    def local_mix(layer, by_lane, by_row, count, read, write):
        pairs = [read(d) for d in range(depth)]
        stride = 1
        cosine, sine = (jnp.broadcast_to(x, (8, lanes))[None] for x in angle(layer, 2))
        re = jnp.stack([p[0] for p in pairs]).reshape(depth, count // 8, 8, lanes)
        im = jnp.stack([p[1] for p in pairs]).reshape(depth, count // 8, 8, lanes)
        while stride < depth:
            re, im = butterfly(re, im, stride, cosine, sine)
            stride *= 2
        re, im = re.reshape(depth, count, lanes), im.reshape(depth, count, lanes)
        for d in range(depth):
            both = dot3(split(jnp.concatenate([re[d], im[d]], 1)), by_lane)
            both = dot3(by_row, split(jnp.concatenate([both[:, :lanes], both[:, lanes:]], 0)))
            write(d, both[:count], both[count:])

    first_tables = tables(0, rows)
    second_tables = tables(1, rows // halves)

    load_en.wait()
    pl.semaphore_wait(barrier, n - 1)
    exchange(en, e_b, 0)
    load_amp.wait()

    def first(d):
        if tiled:
            e = en[pl.ds(d * units, units)].reshape(rows, lanes)
        else:
            e = tmp[0, d]
        sine, cosine = sin_cos(ph[0:1] * e)
        return amp[0, d] * cosine + amp[1, d] * sine, amp[1, d] * cosine - amp[0, d] * sine

    def to_units(d, re, im):
        if tiled:
            for part, x in enumerate((re, im)):
                x = x.reshape(units, halves, step, lanes)
                for h in range(halves):
                    s_a[h, pl.ds(d * units, units), part] = x[:, h]
        else:
            tmp[0, d] = re
            tmp[1, d] = im

    if not tiled:
        for d in range(depth):

            def spread(u, carry):
                tmp[0, d, pl.ds(u * per, per)] = en[d * units + u]
                return carry

            lax.fori_loop(0, units, spread, 0)
    local_mix(0, *first_tables, rows, first, to_units)
    if not tiled:
        for d in range(depth):

            def gather(u, carry):
                for part in range(2):
                    s_a[0, d * units + u, part] = tmp[part, d, pl.ds(u * per, per)]
                return carry

            lax.fori_loop(0, units, gather, 0)

    for h in range(halves):
        exchange(s_a.at[h], b_b.at[h], 1 + h)
    arrived(e_b, n, recv, 0)
    sine, cosine = sin_cos(ph[1:2][None] * e_b[...])
    sn_b[...] = sine
    cs_b[...] = cosine

    for h in range(halves):
        arrived(b_b.at[h], n, recv, 1 + h)
        span = pl.ds(h * step, step)
        re, im = b_b[h, :, 0], b_b[h, :, 1]
        for layer in range(2):
            stride = 1
            while stride < n:
                cosine, sine = (
                    jnp.broadcast_to(x, (step, lanes))[None, None] for x in angle(layer, 3 if stride < nl else 2)
                )
                re, im = butterfly(re, im, stride, cosine, sine)
                stride *= 2
            if layer == 0:
                cosine, sine = cs_b[:, span], sn_b[:, span]
                re, im = re * cosine + im * sine, im * cosine - re * sine
        o_b[h, :, 0] = re
        o_b[h, :, 1] = im
        exchange(o_b.at[h], r_a.at[h], 1 + halves + h)

    def second(h, d):
        if tiled:
            return tuple(
                r_a[h, pl.ds(d * units, units), part].reshape(rows // halves, lanes) for part in range(2)
            )
        return tmp[0, d], tmp[1, d]

    def keep(d, re, im):
        part_done[0, d] = re
        part_done[1, d] = im

    def pass_on(d):
        def one(k, carry):
            to_bank = lax.rem(bank + k, nb)
            pltpu.make_async_remote_copy(
                src_ref=ch.at[d, to_bank],
                dst_ref=m_in.at[bank, d],
                send_sem=send.at[last],
                recv_sem=recv.at[last],
                device_id=(to_bank, lane),
                device_id_type=MESH,
            ).start()
            return carry

        lax.fori_loop(1, nb, one, 0)
        m_in[bank, d] = ch[d, bank]

    def finish(d, re, im):
        if halves == 2:
            cosine, sine = angle(1, 1)
            ur, ui, vr, vi = part_done[0, d], part_done[1, d], re, im
            shape = (units, 1, step, lanes)
            re = [cosine * ur + sine * vi, cosine * vr + sine * ui]
            im = [cosine * ui - sine * vr, cosine * vi - sine * ur]
            re = jnp.concatenate([x.reshape(shape) for x in re], 1).reshape(rows, lanes)
            im = jnp.concatenate([x.reshape(shape) for x in im], 1).reshape(rows, lanes)
        chance = re * re + im * im
        for g in range(nb):
            ch[d, g] = chance[g * piece : (g + 1) * piece]
        out[0, d] = re
        out[1, d] = im
        pass_on(d)

    for h in range(halves):
        arrived(r_a.at[h], n, recv, 1 + halves + h)
        if not tiled:
            for d in range(depth):

                def place(u, carry):
                    for part in range(2):
                        tmp[part, d, pl.ds(u * per, per)] = r_a[h, d * units + u, part]
                    return carry

                lax.fori_loop(0, units, place, 0)
        write = finish if h == halves - 1 else keep
        local_mix(1, *second_tables, rows // halves, functools.partial(second, h), write)

    arrived(m_in, nb, recv, last)
    total = m_in[0]
    for g in range(1, nb):
        total = total + m_in[g]
    marg[...] = total * (1.0 / nb)
    arrived(e_b, n, send, 0)
    for h in range(halves):
        arrived(b_b.at[h], n, send, 1 + h)
        arrived(r_a.at[h], n, send, 1 + halves + h)
    arrived(m_in, nb, send, last)


def on_device(nb, nl, amplitudes, energies, phase_angles, mix_angles):
    _, depth, rows, lanes = amplitudes.shape
    n = nb * nl
    per = depth * rows // n
    halves = 2 if per % 16 == 0 else 1
    piece = rows // nb
    f32 = jnp.float32
    state = pltpu.VMEM((halves, n, 2, per // halves, lanes), f32)
    level = pltpu.VMEM((n, per, lanes), f32)
    vmem = pl.BlockSpec(memory_space=pltpu.VMEM)
    anywhere = pl.BlockSpec(memory_space=pl.ANY)
    whole = pltpu.VMEM((2, depth, rows, lanes), f32)
    return pl.pallas_call(
        functools.partial(kernel, nb, nl, halves),
        name="register",
        out_shape=(pltpu.VMEM(amplitudes.shape, f32), pltpu.VMEM((depth, piece, lanes), f32)),
        in_specs=[anywhere, anywhere, vmem, vmem],
        out_specs=(vmem, vmem),
        scratch_shapes=[
            whole,
            level,
            whole if per % 8 else pltpu.VMEM((1, 1, 8, 128), f32),
            state,
            level,
            state,
            state,
            state,
            level,
            level,
            pltpu.VMEM((2, depth, rows // halves, lanes), f32),
            pltpu.VMEM((depth, nb, piece, lanes), f32),
            pltpu.VMEM((nb, depth, piece, lanes), f32),
            pltpu.SemaphoreType.DMA((2,)),
            pltpu.SemaphoreType.DMA((2 * halves + 2,)),
            pltpu.SemaphoreType.DMA((2 * halves + 2,)),
        ],
        compiler_params=pltpu.CompilerParams(collective_id=0, has_side_effects=True),
    )(amplitudes, energies.reshape(n, per, lanes), phase_angles, mix_angles)


def solution(mesh):
    placed = (P(None, ("bank", "lane"), None, None), P(("bank", "lane"), None, None), P(), P())
    return jax.shard_map(
        functools.partial(on_device, mesh.shape["bank"], mesh.shape["lane"]),
        mesh=mesh,
        in_specs=placed,
        out_specs=(P(None, ("bank", "lane"), None, None), P("lane", "bank", None)),
        check_vma=False,
    )
```

```python
import functools

import jax
import jax.numpy as jnp
from jax import lax
from jax.experimental import pallas as pl
from jax.experimental.pallas import tpu as pltpu
from jax.sharding import PartitionSpec as P

MESH = pl.DeviceIdType.MESH
SIN = (1.0, -1 / 6, 1 / 120, -1 / 5040, 1 / 362880, -1 / 39916800, 1 / 6227020800, -1 / 1307674368000)
COS = (1.0, -1 / 2, 1 / 24, -1 / 720, 1 / 40320, -1 / 3628800, 1 / 479001600, -1 / 87178291200, 1 / 20922789888000)


def series(square, terms):
    total = jnp.full_like(square, terms[-1])
    for term in terms[-2::-1]:
        total = total * square + term
    return total


def sin_cos(turn):
    square = turn * turn
    return turn * series(square, SIN), series(square, COS)


def split(x):
    high = x.astype(jnp.bfloat16)
    return high, (x - high.astype(jnp.float32)).astype(jnp.bfloat16)


def dot3(a, b):
    def one(x, y):
        return lax.dot_general(x, y, (((1,), (0,)), ((), ())), preferred_element_type=jnp.float32)

    return one(a[0], b[0]) + (one(a[1], b[0]) + one(a[0], b[1]))


def turn_table(count, cosine, sine):
    row = lax.broadcasted_iota(jnp.int32, (count, count), 0)
    col = lax.broadcasted_iota(jnp.int32, (count, count), 1)
    apart = row ^ col
    size = jnp.ones((count, count), jnp.float32)
    ones = jnp.zeros((count, count), jnp.int32)
    for place in range(count.bit_length() - 1):
        bit = (apart >> place) & 1
        size = size * jnp.where(bit == 1, sine, cosine)
        ones = ones + bit
    phase = ones & 3
    real = jnp.where(phase == 0, size, jnp.where(phase == 2, -size, 0.0))
    imag = jnp.where(phase == 1, -size, jnp.where(phase == 3, size, 0.0))
    return real, imag


def butterfly(re, im, stride, cosine, sine):
    count, rest = re.shape[0], re.shape[1:]
    parts = (count // (2 * stride), 2, stride) + rest
    re, im = re.reshape(parts), im.reshape(parts)
    ur, vr, ui, vi = re[:, 0], re[:, 1], im[:, 0], im[:, 1]
    new_re = jnp.stack([cosine * ur + sine * vi, cosine * vr + sine * ui], axis=1)
    new_im = jnp.stack([cosine * ui - sine * vr, cosine * vi - sine * ur], axis=1)
    return new_re.reshape((count,) + rest), new_im.reshape((count,) + rest)


def kernel(
    nb, nl, halves, amp_hbm, en_hbm, ph, mix, out, marg,
    amp, en, tmp, s_a, e_b, b_b, o_b, r_a, cs_b, sn_b, part_done, ch, m_in, load, send, recv,
):
    n = nb * nl
    depth, rows, lanes = amp.shape[1:]
    per = en.shape[1]
    step = per // halves
    tiled = per % 8 == 0
    units = rows // per
    piece = rows // nb
    last = 2 * halves + 1
    bank, lane = lax.axis_index("bank"), lax.axis_index("lane")
    me = bank * nl + lane

    load_en = pltpu.make_async_copy(en_hbm, en, load.at[0])
    load_amp = pltpu.make_async_copy(amp_hbm, amp, load.at[1])
    load_en.start()
    load_amp.start()
    barrier = pltpu.get_barrier_semaphore()

    def partner(k):
        return lax.rem(bank + nb - lax.rem(k, nb), nb), lax.rem(lane + k // nb, nl)

    def greet(k, carry):
        pl.semaphore_signal(barrier, 1, device_id=partner(k), device_id_type=MESH)
        return carry

    lax.fori_loop(1, n, greet, 0)

    def exchange(src, dst, which):
        def one(k, carry):
            to_bank, to_lane = partner(k)
            pltpu.make_async_remote_copy(
                src_ref=src.at[to_bank * nl + to_lane],
                dst_ref=dst.at[me],
                send_sem=send.at[which],
                recv_sem=recv.at[which],
                device_id=(to_bank, to_lane),
                device_id_type=MESH,
            ).start()
            return carry

        lax.fori_loop(1, n, one, 0)
        dst[me] = src[me]

    def arrived(dst, count, sems, which):
        most = dst.at[pl.ds(0, count - 1)]
        pltpu.make_async_copy(most, most, sems.at[which]).wait()

    cosines, sines = jnp.cos(mix[...]), jnp.sin(mix[...])

    def angle(layer, group):
        return cosines[layer : layer + 1, group : group + 1], sines[layer : layer + 1, group : group + 1]

    def tables(layer, count):
        real, imag = turn_table(lanes, *angle(layer, 0))
        by_lane = split(jnp.concatenate([jnp.concatenate([real, imag], 1), jnp.concatenate([-imag, real], 1)], 0))
        real, imag = turn_table(count, *angle(layer, 1))
        by_row = split(jnp.concatenate([jnp.concatenate([real, -imag], 1), jnp.concatenate([imag, real], 1)], 0))
        return by_lane, by_row

    def local_mix(layer, by_lane, by_row, count, read, write):
        pairs = [read(d) for d in range(depth)]
        stride = 1
        cosine, sine = (jnp.broadcast_to(x, (8, lanes))[None] for x in angle(layer, 2))
        re = jnp.stack([p[0] for p in pairs]).reshape(depth, count // 8, 8, lanes)
        im = jnp.stack([p[1] for p in pairs]).reshape(depth, count // 8, 8, lanes)
        while stride < depth:
            re, im = butterfly(re, im, stride, cosine, sine)
            stride *= 2
        re, im = re.reshape(depth, count, lanes), im.reshape(depth, count, lanes)
        for d in range(depth):
            both = dot3(split(jnp.concatenate([re[d], im[d]], 1)), by_lane)
            both = dot3(by_row, split(jnp.concatenate([both[:, :lanes], both[:, lanes:]], 0)))
            write(d, both[:count], both[count:])

    first_tables = tables(0, rows)
    second_tables = tables(1, rows // halves)

    load_en.wait()
    pl.semaphore_wait(barrier, n - 1)
    exchange(en, e_b, 0)
    load_amp.wait()

    def first(d):
        if tiled:
            e = en[pl.ds(d * units, units)].reshape(rows, lanes)
        else:
            e = tmp[0, d]
        sine, cosine = sin_cos(ph[0:1] * e)
        return amp[0, d] * cosine + amp[1, d] * sine, amp[1, d] * cosine - amp[0, d] * sine

    def to_units(d, re, im):
        if tiled:
            for part, x in enumerate((re, im)):
                x = x.reshape(units, halves, step, lanes)
                for h in range(halves):
                    s_a[h, pl.ds(d * units, units), part] = x[:, h]
        else:
            tmp[0, d] = re
            tmp[1, d] = im

    if not tiled:
        for d in range(depth):

            def spread(u, carry):
                tmp[0, d, pl.ds(u * per, per)] = en[d * units + u]
                return carry

            lax.fori_loop(0, units, spread, 0)
    local_mix(0, *first_tables, rows, first, to_units)
    if not tiled:
        for d in range(depth):

            def gather(u, carry):
                for part in range(2):
                    s_a[0, d * units + u, part] = tmp[part, d, pl.ds(u * per, per)]
                return carry

            lax.fori_loop(0, units, gather, 0)

    for h in range(halves):
        exchange(s_a.at[h], b_b.at[h], 1 + h)
    arrived(e_b, n, recv, 0)
    sine, cosine = sin_cos(ph[1:2][None] * e_b[...])
    sn_b[...] = sine
    cs_b[...] = cosine

    for h in range(halves):
        arrived(b_b.at[h], n, recv, 1 + h)
        span = pl.ds(h * step, step)
        re, im = b_b[h, :, 0], b_b[h, :, 1]
        for layer in range(2):
            stride = 1
            while stride < n:
                cosine, sine = (
                    jnp.broadcast_to(x, (step, lanes))[None, None] for x in angle(layer, 3 if stride < nl else 2)
                )
                re, im = butterfly(re, im, stride, cosine, sine)
                stride *= 2
            if layer == 0:
                cosine, sine = cs_b[:, span], sn_b[:, span]
                re, im = re * cosine + im * sine, im * cosine - re * sine
        o_b[h, :, 0] = re
        o_b[h, :, 1] = im
        exchange(o_b.at[h], r_a.at[h], 1 + halves + h)

    def second(h, d):
        if tiled:
            return tuple(
                r_a[h, pl.ds(d * units, units), part].reshape(rows // halves, lanes) for part in range(2)
            )
        return tmp[0, d], tmp[1, d]

    def keep(d, re, im):
        part_done[0, d] = re
        part_done[1, d] = im

    def pass_on(d):
        def one(k, carry):
            to_bank = lax.rem(bank + k, nb)
            pltpu.make_async_remote_copy(
                src_ref=ch.at[d, to_bank],
                dst_ref=m_in.at[bank, d],
                send_sem=send.at[last],
                recv_sem=recv.at[last],
                device_id=(to_bank, lane),
                device_id_type=MESH,
            ).start()
            return carry

        lax.fori_loop(1, nb, one, 0)
        m_in[bank, d] = ch[d, bank]

    def finish(d, re, im):
        if halves == 2:
            cosine, sine = angle(1, 1)
            ur, ui, vr, vi = part_done[0, d], part_done[1, d], re, im
            shape = (units, 1, step, lanes)
            re = [cosine * ur + sine * vi, cosine * vr + sine * ui]
            im = [cosine * ui - sine * vr, cosine * vi - sine * ur]
            re = jnp.concatenate([x.reshape(shape) for x in re], 1).reshape(rows, lanes)
            im = jnp.concatenate([x.reshape(shape) for x in im], 1).reshape(rows, lanes)
        chance = re * re + im * im
        for g in range(nb):
            ch[d, g] = chance[g * piece : (g + 1) * piece]
        out[0, d] = re
        out[1, d] = im
        pass_on(d)

    for h in range(halves):
        arrived(r_a.at[h], n, recv, 1 + halves + h)
        if not tiled:
            for d in range(depth):

                def place(u, carry):
                    for part in range(2):
                        tmp[part, d, pl.ds(u * per, per)] = r_a[h, d * units + u, part]
                    return carry

                lax.fori_loop(0, units, place, 0)
        write = finish if h == halves - 1 else keep
        local_mix(1, *second_tables, rows // halves, functools.partial(second, h), write)

    arrived(m_in, nb, recv, last)
    total = m_in[0]
    for g in range(1, nb):
        total = total + m_in[g]
    marg[...] = total * (1.0 / nb)
    arrived(e_b, n, send, 0)
    for h in range(halves):
        arrived(b_b.at[h], n, send, 1 + h)
        arrived(r_a.at[h], n, send, 1 + halves + h)
    arrived(m_in, nb, send, last)


def on_device(nb, nl, amplitudes, energies, phase_angles, mix_angles):
    _, depth, rows, lanes = amplitudes.shape
    n = nb * nl
    per = depth * rows // n
    halves = 2 if per % 16 == 0 else 1
    piece = rows // nb
    f32 = jnp.float32
    state = pltpu.VMEM((halves, n, 2, per // halves, lanes), f32)
    level = pltpu.VMEM((n, per, lanes), f32)
    vmem = pl.BlockSpec(memory_space=pltpu.VMEM)
    anywhere = pl.BlockSpec(memory_space=pl.ANY)
    whole = pltpu.VMEM((2, depth, rows, lanes), f32)
    return pl.pallas_call(
        functools.partial(kernel, nb, nl, halves),
        name="register",
        out_shape=(pltpu.VMEM(amplitudes.shape, f32), pltpu.VMEM((depth, piece, lanes), f32)),
        in_specs=[anywhere, anywhere, vmem, vmem],
        out_specs=(vmem, vmem),
        scratch_shapes=[
            whole,
            level,
            whole if per % 8 else pltpu.VMEM((1, 1, 8, 128), f32),
            state,
            level,
            state,
            state,
            state,
            level,
            level,
            pltpu.VMEM((2, depth, rows // halves, lanes), f32),
            pltpu.VMEM((depth, nb, piece, lanes), f32),
            pltpu.VMEM((nb, depth, piece, lanes), f32),
            pltpu.SemaphoreType.DMA((2,)),
            pltpu.SemaphoreType.DMA((2 * halves + 2,)),
            pltpu.SemaphoreType.DMA((2 * halves + 2,)),
        ],
        compiler_params=pltpu.CompilerParams(collective_id=0, has_side_effects=True),
    )(amplitudes, energies.reshape(n, per, lanes), phase_angles, mix_angles)


def solution(mesh):
    placed = (P(None, ("bank", "lane"), None, None), P(("bank", "lane"), None, None), P(), P())
    return jax.shard_map(
        functools.partial(on_device, mesh.shape["bank"], mesh.shape["lane"]),
        mesh=mesh,
        in_specs=placed,
        out_specs=(P(None, ("bank", "lane"), None, None), P("lane", "bank", None)),
        check_vma=False,
    )
```
